32 devices in a mesh: groups: 2 (over y), dom: 4 (over z), sub: 2 (over x), field: 2 (over core).
Axes of the slice: x: 2, y: 2, z: 4, core: 2. Of those that a mesh axis runs over, the one named last changes fastest.
Arguments:
- background: float32 [3, 65536], P(None, ('groups', 'dom', 'sub')), parts along dimension 1, may hold values from -6 to 6
- obs_weight: float32 [65536], P(('groups', 'dom', 'sub')), parts along dimension 0, may hold values from 0.02 to 0.2
- connect: int32 [10, 32768], P(None, ('groups', 'dom', 'sub', 'field')), parts along dimension 1, may hold values from 0 to 5631, as said below
- live_blocks: int32 [32], P(('groups', 'dom', 'sub', 'field')), parts along dimension 0, may hold values from 2 to 8, as said below
- elem_scale: float32 [32768], P(('groups', 'dom', 'sub', 'field')), parts along dimension 0, may hold values from 0.5 to 2
- reg_weight: float32 [32768], P(('groups', 'dom', 'sub', 'field')), parts along dimension 0, may hold values from 0.2 to 2
- iterate: float32 [32768], P(('groups', 'dom', 'sub', 'field')), parts along dimension 0, may hold values from -6 to 6
- residual: float32 [32768], P(('groups', 'dom', 'sub', 'field')), parts along dimension 0, may hold values from -30 to 30
- direction: float32 [32768], P(('groups', 'dom', 'sub', 'field')), parts along dimension 0, may hold values from -30 to 30
- send_nodes: int32 [16, 3, 2, 256], P(('groups', 'dom', 'sub')), parts along dimension 0, may hold values from 0 to 4095, as said below
- send_count: int32 [16, 3, 2], P(('groups', 'dom', 'sub')), parts along dimension 0, may hold values from 0 to 256, as said below
- ref_stiff: float32 [30, 30], replicated, may hold values from -1.05 to 4.05, as said below
Outputs:
- iterate_next: float32 [32768], P(('groups', 'dom', 'sub', 'field')), parts along dimension 0
- residual_next: float32 [32768], P(('groups', 'dom', 'sub', 'field')), parts along dimension 0
- direction_next: float32 [32768], P(('groups', 'dom', 'sub', 'field')), parts along dimension 0
The draws below stay inside these ranges and needn't reach their ends.
There are 2 independent parts, one for each index of `groups`. The reference program is written for one: setup_inputs(seed, part) draws one part's arguments, and reference() takes and returns one part's arrays. A program takes and returns all parts, laid end to end along the dimension named above; an argument that names none is the same for every part. Nothing has to cross between parts.
Inputs may be any that keep to these rules, and one draw needn't show every extreme that they name: `send_nodes`: for every link the first send_count slots hold distinct owned nodes; later slots are padding. `send_count`: links go only to partitions of dom index d - 1, d or d + 1 and never to the sender itself or past the ends of dom; some link is full with 256 slots. `connect`: entries from 4096 on name ghost slots that are live slots of their owner's link. `live_blocks`: live blocks fill a device's slots from its first one; some device has 8. `ref_stiff`: Symmetric.
All inputs are finite; a program needn't handle non-finite values.
Results may differ from the reference program's by a relative error of at most 0.00005.
Values sent between devices are 32-bit elements; how exact they have to be, the bound alone decides.
A program may use at most 64 MiB of HBM per device.

```python
import math
import jax
import jax.numpy as jnp
from jax import lax

NLOC = 4096
MAXB = 8
BLK = 128
LINK = 256
PARTITIONS = 8
CORES = 16
NODES = 32768
ELEMS = 16384
N_DOM = 4
N_SUB = 2
N_FIELD = 2


def interface_layout(key):
    salted = jax.random.fold_in(key, 17)
    linked_key, amount_key, chosen_key, start_key, stride_key = jax.random.split(salted, 5)
    partition = jnp.arange(PARTITIONS, dtype=jnp.int32)
    dom_index = partition // N_SUB
    sub_index = partition % N_SUB
    offset = jnp.arange(3, dtype=jnp.int32)
    target_sub = jnp.arange(N_SUB, dtype=jnp.int32)
    target_dom = dom_index[:, None, None] + offset[None, :, None] - 1
    itself = (offset[None, :, None] == 1) & (target_sub[None, None, :] == sub_index[:, None, None])
    exists = (target_dom >= 0) & (target_dom < N_DOM) & jnp.logical_not(itself)
    linked = jax.random.randint(linked_key, (PARTITIONS, 3, N_SUB), 0, 4) > 0
    amount = jax.random.randint(amount_key, (PARTITIONS, 3, N_SUB), LINK // 4, LINK + 1)
    counts = jnp.where(exists & linked, amount, 0)
    chosen = jax.random.randint(chosen_key, (), 0, PARTITIONS)
    counts = counts.at[chosen, 1, (chosen % N_SUB + 1) % N_SUB].set(LINK)
    starts = jax.random.randint(start_key, (PARTITIONS, 3, N_SUB, 1), 0, NLOC)
    strides = jax.random.randint(stride_key, (PARTITIONS, 3, N_SUB, 1), 1, NLOC // LINK + 1)
    sent_nodes = (starts + jnp.arange(LINK, dtype=jnp.int32)[None, None, None, :] * strides) % NLOC
    return (sent_nodes.astype(jnp.int32), counts.astype(jnp.int32))


def draw_send_nodes(key, part):
    sent_nodes, counts = interface_layout(key)
    return sent_nodes


def draw_send_count(key, part):
    sent_nodes, counts = interface_layout(key)
    return counts


def draw_connect(key, part):
    sent_nodes, counts = interface_layout(key)
    salted = jax.random.fold_in(key, 29)
    local_key, offset_key, source_key, position_key, choose_key = jax.random.split(salted, 5)
    layout_shape = (10, ELEMS)
    element = jnp.arange(ELEMS, dtype=jnp.int32)
    partition = element // (N_FIELD * MAXB * BLK)
    dom_index = partition // N_SUB
    sub_index = jnp.broadcast_to((partition % N_SUB)[None, :], layout_shape)
    local_pick = jax.random.randint(local_key, layout_shape, 0, NLOC)
    offset = jax.random.randint(offset_key, layout_shape, 0, 3)
    source_sub = jax.random.randint(source_key, layout_shape, 0, N_SUB)
    position = jax.random.randint(position_key, layout_shape, 0, LINK)
    wanted = jax.random.randint(choose_key, layout_shape, 0, 4) == 0
    raw_dom = dom_index[None, :] + offset - 1
    inside = (raw_dom >= 0) & (raw_dom < N_DOM)
    owner_part = jnp.clip(raw_dom, 0, N_DOM - 1) * N_SUB + source_sub
    usable = wanted & inside & (position < counts[owner_part, 2 - offset, sub_index])
    ghost_pick = NLOC + (offset * N_SUB + source_sub) * LINK + position
    return jnp.where(usable, ghost_pick, local_pick).astype(jnp.int32)


def draw_live_blocks(key, part):
    salted = jax.random.fold_in(key, 41)
    amount_key, chosen_key = jax.random.split(salted)
    counts = jax.random.randint(amount_key, (CORES,), MAXB // 4, MAXB // 2 + 1)
    chosen = jax.random.randint(chosen_key, (), 0, CORES)
    return counts.at[chosen].set(MAXB).astype(jnp.int32)


def rising_field(key, salt):
    salted = jax.random.fold_in(key, salt)
    scale_key, value_key = jax.random.split(salted)
    position = jnp.arange(ELEMS, dtype=jnp.float32) / ELEMS
    spread = jnp.exp(jax.random.uniform(scale_key, (ELEMS,), jnp.float32, 0.0, jnp.log(10.0)))
    scales = (1.0 + 2.0 * position) * spread / 4.0
    baseline = jnp.clip(jax.random.normal(value_key, (ELEMS,), jnp.float32), -4.0, 4.0)
    return (baseline * scales).astype(jnp.float32)


def draw_residual(key, part):
    return rising_field(key, 61)


def draw_direction(key, part):
    return rising_field(key, 67)


def draw_ref_stiff(key, part):
    salted = jax.random.fold_in(key, 53)
    diagonal_key, coupling_key = jax.random.split(salted)
    diagonal = jax.random.uniform(diagonal_key, (30,), jnp.float32, 1.5, 3.0)
    coupling = jnp.clip(jax.random.normal(coupling_key, (30, 30), jnp.float32), -3.0, 3.0)
    symmetric = 0.35 * (coupling + coupling.T) / 2.0
    identity = jnp.eye(30, dtype=jnp.float32)
    return (symmetric * (1.0 - identity) + identity * diagonal[None, :]).astype(jnp.float32)


def shard_levels(own_key, extent, cuts, smallest, high):
    def one(axis_at, shards_of):
        draws = jax.random.uniform(jax.random.fold_in(jax.random.fold_in(own_key, 6), axis_at), (shards_of,), jnp.float32, smallest / len(cuts), high / len(cuts))
        return jnp.repeat(jnp.exp(draws), extent[axis_at] // shards_of).reshape((-1,) + (1,) * (len(extent) - axis_at - 1))

    level = one(*cuts[0])
    for cut in cuts[1:]:
        level = level * one(*cut)
    return level


def bell_draw(own_key, extent, deviation, reach, pieces=(), kind=jnp.bfloat16):
    gain = shard_levels(own_key, extent, pieces, -0.22, 0.18) if pieces else 1.0
    drawn = jax.random.normal(own_key, extent, jnp.float32) * deviation * gain
    return jnp.minimum(jnp.maximum(drawn, -reach), reach).astype(kind)


def setup_inputs(seed: int = 0, part: int = 0) -> dict:
    key_list = jax.random.split(jax.random.key(seed), 13)
    own_keys = jax.random.split(jax.random.fold_in(key_list[12], part), 13)
    background = bell_draw(own_keys[0], (3, NODES), 1.0, 6.0, ((1, 8),), jnp.float32)
    obs_weight = jnp.clip(jnp.exp(math.log(0.2) - 2.3025851 * jax.random.uniform(own_keys[1], (NODES,), jnp.float32) ** shard_levels(own_keys[1], (NODES,), ((0, 8),), -0.2, 0.2)), 0.02, 0.2)
    connect = draw_connect(jax.random.fold_in(jax.random.fold_in(key_list[12], part), 71), part)
    live_blocks = draw_live_blocks(jax.random.fold_in(jax.random.fold_in(key_list[12], part), 71), part)
    elem_scale = jnp.clip(jnp.exp(math.log(2.0) - 1.3862944 * jax.random.uniform(own_keys[4], (ELEMS,), jnp.float32) ** shard_levels(own_keys[4], (ELEMS,), ((0, 16),), -0.2, 0.2)), 0.5, 2.0)
    reg_weight = jnp.clip(jnp.exp(math.log(2.0) - 2.3025851 * jax.random.uniform(own_keys[5], (ELEMS,), jnp.float32) ** shard_levels(own_keys[5], (ELEMS,), ((0, 16),), -0.2, 0.2)), 0.2, 2.0)
    iterate = bell_draw(own_keys[6], (ELEMS,), 1.0, 6.0, ((0, 16),), jnp.float32)
    residual = draw_residual(jax.random.fold_in(jax.random.fold_in(key_list[12], part), 71), part)
    direction = draw_direction(jax.random.fold_in(jax.random.fold_in(key_list[12], part), 71), part)
    send_nodes = draw_send_nodes(jax.random.fold_in(jax.random.fold_in(key_list[12], part), 71), part)
    send_count = draw_send_count(jax.random.fold_in(jax.random.fold_in(key_list[12], part), 71), part)
    ref_stiff = draw_ref_stiff(jax.random.fold_in(key_list[12], 71), part)
    return dict(background=background, obs_weight=obs_weight, connect=connect, live_blocks=live_blocks, elem_scale=elem_scale, reg_weight=reg_weight, iterate=iterate, residual=residual, direction=direction, send_nodes=send_nodes, send_count=send_count, ref_stiff=ref_stiff)


def global_nodes(connect, send_nodes, send_count):
    element_count = connect.shape[1]
    element = jnp.arange(element_count, dtype=jnp.int32)
    partition = element // (N_FIELD * MAXB * BLK)
    dom_index = partition // N_SUB
    sub_index = jnp.broadcast_to((partition % N_SUB)[None, :], connect.shape)
    ghosted = jnp.maximum(connect - NLOC, 0)
    offset = ghosted // (N_SUB * LINK)
    source_sub = (ghosted // LINK) % N_SUB
    position = ghosted % LINK
    raw_dom = dom_index[None, :] + offset - 1
    inside = (raw_dom >= 0) & (raw_dom < N_DOM)
    owner_part = (jnp.clip(raw_dom, 0, N_DOM - 1) * N_SUB + source_sub).astype(jnp.int32)
    slot_node = send_nodes[owner_part, 2 - offset, sub_index, position]
    remote = owner_part * NLOC + slot_node
    remote_ok = inside & (position < send_count[owner_part, 2 - offset, sub_index])
    local_ok = connect < NLOC
    node_map = jnp.where(local_ok, partition[None, :] * NLOC + connect, remote).astype(jnp.int32)
    valid_mask = (local_ok | remote_ok).astype(jnp.float32)
    return node_map, valid_mask


def reference(background, obs_weight, connect, live_blocks, elem_scale, reg_weight, iterate, residual, direction, send_nodes, send_count, ref_stiff):
    element_count = connect.shape[1]
    element = jnp.arange(element_count, dtype=jnp.int32)
    device = element // (MAXB * BLK)
    within = element % (MAXB * BLK)
    live_mask = (within < BLK * live_blocks[device]).astype(jnp.float32)
    search = live_mask * direction
    remain = live_mask * residual
    guess = live_mask * iterate
    node_map, valid_mask = global_nodes(connect, send_nodes, send_count)
    element_state = (background[:, node_map] * valid_mask[None]).reshape(30, element_count)
    coupled = (live_mask * elem_scale)[None, :] * jnp.dot(ref_stiff, element_state, precision=lax.Precision.HIGHEST)
    terms = (search[None, :] * coupled).reshape(3, 10, element_count) * valid_mask[None]
    assembled = jnp.zeros(background.shape, jnp.float32).at[:, node_map.reshape(-1)].add(terms.reshape(3, -1))
    weighted = obs_weight[None, :] * assembled
    pulled = weighted[:, node_map] * valid_mask[None]
    hess_search = jnp.sum(coupled.reshape(3, 10, element_count) * pulled, axis=(0, 1)) + reg_weight * search
    squared_before = jnp.sum(remain * remain)
    curvature_sum = jnp.sum(search * hess_search)
    step_length = squared_before / curvature_sum
    iterate_next = guess + step_length * search
    residual_next = remain - step_length * hess_search
    squared_after = jnp.sum(residual_next * residual_next)
    direction_next = residual_next + (squared_after / squared_before) * search
    return iterate_next, residual_next, direction_next
```

```python
import functools

import jax
import jax.numpy as jnp
from jax import lax
from jax.experimental import pallas as pl
from jax.experimental.pallas import tpu as pltpu
from jax.sharding import PartitionSpec as P

BLK = 128
LANES = 128
F32 = jnp.float32
BF16 = jnp.bfloat16
MESH = pl.DeviceIdType.MESH


def split(values):
    high = values.astype(BF16)
    return high, (values - high.astype(F32)).astype(BF16)


def low_hot(index):
    rows = lax.broadcasted_iota(jnp.int32, (LANES, index.shape[1]), 0)
    return jnp.where(rows == (index & (LANES - 1)), 1.0, 0.0).astype(BF16)


def high_mask(index, rows):
    return lax.broadcasted_iota(jnp.int32, (rows, index.shape[1]), 0) == (index >> 7)


def picked(table, rows, index):
    hot = low_hot(index)
    wide = jnp.dot(table, jnp.concatenate([hot, hot], axis=0), preferred_element_type=F32)
    mask = high_mask(index, rows)
    return [jnp.where(mask, wide[c * rows : (c + 1) * rows], 0.0) for c in range(3)]


def spread(values, index, rows):
    mask = high_mask(index, rows)
    pieces = [split(v) for v in values]
    blocks = []
    for p in range(2):
        for c in range(3):
            piece = jnp.broadcast_to(pieces[c][p].astype(F32), mask.shape)
            blocks.append(jnp.where(mask, piece, 0.0).astype(BF16))
    return lax.dot_general(
        jnp.concatenate(blocks, axis=0),
        low_hot(index),
        (((1,), (1,)), ((), ())),
        preferred_element_type=F32,
    )


def kernel(
    doms,
    subs,
    fields,
    stages,
    background,
    obs_weight,
    connect,
    live_blocks,
    elem_scale,
    reg_weight,
    iterate,
    residual,
    direction,
    send_nodes,
    send_count,
    ref_stiff,
    iterate_next,
    residual_next,
    direction_next,
    table_f,
    table,
    state,
    coupled,
    acc,
    own,
    own_in,
    out_a,
    in_a,
    out_b,
    in_b,
    ret,
    ret_in,
    red,
    red_in,
    sems_a,
    sems_b,
    sems_r,
    sems_x,
    sems_s,
):
    d, s, f = (lax.axis_index(a) for a in ("dom", "sub", "field"))
    elements = connect.shape[1]
    link = send_nodes.shape[3]
    own_rows = obs_weight.shape[0]
    rows = table_f.shape[1]
    per_link = link // LANES
    links = [(o, t) for o in range(3) for t in range(subs) if (o, t) != (1, 0)]

    def at(dd, ds, df):
        return {
            "dom": lax.rem(d + dd + doms, doms),
            "sub": lax.rem(s + ds, subs),
            "field": lax.rem(f + df, fields),
        }

    def when(o, step):
        if o == 0:
            pl.when(d > 0)(step)
        elif o == 2:
            pl.when(d < doms - 1)(step)
        else:
            step()

    greeted = {(dd % doms, ds, df) for dd in (-1, 0, 1) for ds in range(subs) for df in range(fields)}
    for stage in stages:
        greeted |= set(stage)
    greeted = sorted(greeted - {(0, 0, 0)})

    in_a[...] = jnp.zeros_like(in_a)
    in_b[...] = jnp.zeros_like(in_b)
    ret_in[...] = jnp.zeros_like(ret_in)
    barrier = pltpu.get_barrier_semaphore()
    for offset in greeted:
        pl.semaphore_signal(barrier, inc=1, device_id=at(*offset), device_id_type=MESH)

    table_f[...] = jnp.zeros_like(table_f)
    for r in range(own_rows):
        table_f[:, r, :] = background[:, r * LANES : (r + 1) * LANES]

    def fill_table(part):
        for c in range(3):
            high, low = split(table_f[c])
            table[c * rows : (c + 1) * rows, :LANES] = high
            table[c * rows : (c + 1) * rows, LANES:] = low

    def outbound(out):
        for o in range(3):
            for t in range(subs):
                index = send_nodes[0, o, t : t + 1, :]
                slot = lax.broadcasted_iota(jnp.int32, index.shape, 1)
                open_slot = jnp.where(slot < send_count[0, o, t], 1.0, 0.0)
                for c, wide in enumerate(picked(table[...], rows, index)):
                    out[o * subs + t, c : c + 1, :] = open_slot * jnp.sum(wide, axis=0, keepdims=True)

    def ghost_copy(o, t, out, landing, sems):
        return pltpu.make_async_remote_copy(
            src_ref=out.at[o * subs + lax.rem(s + t, subs)],
            dst_ref=landing.at[(2 - o) * subs + s],
            send_sem=sems.at[0, o * subs + t],
            recv_sem=sems.at[1, (2 - o) * subs + (subs - t) % subs],
            device_id=at(o - 1, t, 0),
            device_id_type=MESH,
        )

    def ghost_arrival(o, t, out, landing, sems):
        return pltpu.make_async_remote_copy(
            src_ref=out.at[o * subs + lax.rem(s + t, subs)],
            dst_ref=landing.at[o * subs + lax.rem(s + t, subs)],
            send_sem=sems.at[0, o * subs + t],
            recv_sem=sems.at[1, o * subs + t],
            device_id=at(o - 1, t, 0),
            device_id_type=MESH,
        )

    def exchange(out, landing, sems):
        for o, t in links:
            when(o, lambda o=o, t=t: ghost_copy(o, t, out, landing, sems).start())
        for o, t in links:
            when(o, lambda o=o, t=t: ghost_arrival(o, t, out, landing, sems).wait_recv())
        for o, t in links:
            when(o, lambda o=o, t=t: ghost_copy(o, t, out, landing, sems).wait_send())

    def ghosts_in(landing):
        for q in range(3 * subs):
            for h in range(per_link):
                table_f[:, own_rows + q * per_link + h, :] = landing[q, :, h * LANES : (h + 1) * LANES]

    fill_table(0)
    outbound(out_a)
    pl.semaphore_wait(barrier, len(greeted))
    exchange(out_a, in_a, sems_a)
    ghosts_in(in_a)
    fill_table(1)

    element = lax.broadcasted_iota(jnp.int32, (1, elements), 1)
    live = jnp.where(element < BLK * live_blocks[0], 1.0, 0.0)
    search = live * direction[...]
    remain = live * residual[...]
    guess = live * iterate[...]
    nodes = connect.shape[0]

    def pull(k, carry):
        index = connect[pl.ds(k, 1), :]
        for c, wide in enumerate(picked(table[...], rows, index)):
            state[pl.ds(c * nodes + k, 1), :] = jnp.sum(wide, axis=0, keepdims=True)
        return carry

    lax.fori_loop(0, nodes, pull, 0)
    coupled[...] = (live * elem_scale[...]) * jnp.dot(
        ref_stiff[...], state[...], precision=lax.Precision.HIGHEST, preferred_element_type=F32
    )

    acc[...] = jnp.zeros_like(acc)

    def push(k, carry):
        index = connect[pl.ds(k, 1), :]
        terms = [search * coupled[pl.ds(c * nodes + k, 1), :] for c in range(3)]
        acc[...] += spread(terms, index, rows)
        return carry

    lax.fori_loop(0, nodes, push, 0)
    for c in range(3):
        total = acc[c * rows : (c + 1) * rows, :] + acc[(3 + c) * rows : (4 + c) * rows, :]
        own[c] = total[:own_rows]
        for q in range(3 * subs):
            for h in range(per_link):
                r = own_rows + q * per_link + h
                ret[q, c : c + 1, h * LANES : (h + 1) * LANES] = total[r : r + 1]

    def ret_copy(o, t, g):
        return pltpu.make_async_remote_copy(
            src_ref=ret.at[o * subs + lax.rem(s + t, subs)],
            dst_ref=ret_in.at[g, (2 - o) * subs + s],
            send_sem=sems_r.at[0, g, o * subs + t],
            recv_sem=sems_r.at[1, g, (2 - o) * subs + (subs - t) % subs],
            device_id=at(o - 1, t, g),
            device_id_type=MESH,
        )

    def ret_arrival(o, t, g):
        return pltpu.make_async_remote_copy(
            src_ref=ret.at[o * subs + lax.rem(s + t, subs)],
            dst_ref=ret_in.at[g, o * subs + lax.rem(s + t, subs)],
            send_sem=sems_r.at[0, g, o * subs + t],
            recv_sem=sems_r.at[1, g, o * subs + t],
            device_id=at(o - 1, t, g),
            device_id_type=MESH,
        )

    def own_copy(g):
        return pltpu.make_async_remote_copy(
            src_ref=own,
            dst_ref=own_in.at[g - 1],
            send_sem=sems_x.at[0, g - 1],
            recv_sem=sems_x.at[1, g - 1],
            device_id=at(0, 0, g),
            device_id_type=MESH,
        )

    for o, t in links:
        for g in range(fields):
            when(o, lambda o=o, t=t, g=g: ret_copy(o, t, g).start())
    for g in range(1, fields):
        own_copy(g).start()
    for o, t in links:
        for g in range(fields):
            when(o, lambda o=o, t=t, g=g: ret_arrival(o, t, g).wait_recv())
    landed = None
    for o in range(3):
        for t in range(subs):
            q = o * subs + t
            index = send_nodes[0, o, t : t + 1, :]
            slot = lax.broadcasted_iota(jnp.int32, index.shape, 1)
            open_slot = jnp.where(slot < send_count[0, o, t], 1.0, 0.0)
            sums = ret_in[0, q]
            for g in range(1, fields):
                sums = sums + ret_in[g, q]
            part = spread([open_slot * sums[c : c + 1] for c in range(3)], index, own_rows)
            landed = part if landed is None else landed + part
    for g in range(1, fields):
        own_copy(g).wait_recv()
    for c in range(3):
        assembled = own[c]
        for g in range(1, fields):
            assembled = assembled + own_in[g - 1, c]
        assembled = assembled + landed[c * own_rows : (c + 1) * own_rows]
        assembled = assembled + landed[(3 + c) * own_rows : (4 + c) * own_rows]
        table_f[c, :own_rows, :] = obs_weight[...] * assembled

    fill_table(0)
    outbound(out_b)
    exchange(out_b, in_b, sems_b)
    ghosts_in(in_b)
    fill_table(1)

    def back(k, total):
        index = connect[pl.ds(k, 1), :]
        for c, wide in enumerate(picked(table[...], rows, index)):
            total = total + coupled[pl.ds(c * nodes + k, 1), :] * jnp.sum(wide, axis=0, keepdims=True)
        return total

    hess = lax.fori_loop(0, nodes, back, jnp.zeros((1, elements), F32)) + reg_weight[...] * search

    def lane_sums(values):
        total = values[:, :LANES]
        for e in range(LANES, elements, LANES):
            total = total + values[:, e : e + LANES]
        return total

    red[0] = jnp.concatenate(
        [lane_sums(v) for v in (remain * remain, search * hess, remain * hess, hess * hess)]
        + [jnp.zeros((4, LANES), F32)],
        axis=0,
    )
    first = 0
    for n, stage in enumerate(stages):

        def red_copy(i, offset, n=n, first=first):
            return pltpu.make_async_remote_copy(
                src_ref=red.at[n],
                dst_ref=red_in.at[first + i],
                send_sem=sems_s.at[0, first + i],
                recv_sem=sems_s.at[1, first + i],
                device_id=at(*offset),
                device_id_type=MESH,
            )

        for i, offset in enumerate(stage):
            red_copy(i, offset).start()
        total = red[n]
        for i, offset in enumerate(stage):
            red_copy(i, offset).wait_recv()
            total = total + red_in[first + i]
        for i, offset in enumerate(stage):
            red_copy(i, offset).wait_send()
        red[n + 1] = total
        first += len(stage)
    sums = jnp.sum(red[len(stages)], axis=1, keepdims=True)
    before, curvature, cross, image = (sums[i : i + 1] for i in range(4))
    step = before / curvature
    after = before - 2.0 * step * cross + step * step * image
    remain_next = remain - step * hess
    iterate_next[...] = guess + step * search
    residual_next[...] = remain_next
    direction_next[...] = remain_next + (after / before) * search
    for o, t in links:
        for g in range(fields):
            when(o, lambda o=o, t=t, g=g: ret_copy(o, t, g).wait_send())
    for g in range(1, fields):
        own_copy(g).wait_send()


def solution(mesh):
    doms, subs, fields = (mesh.shape[a] for a in ("dom", "sub", "field"))
    whole = [(a, b, c) for a in range(doms) for b in range(subs) for c in range(fields)]
    whole = whole[1:]
    if len(whole) < 32:
        stages = [whole]
    else:
        stages = [[w for w in whole if w[0] == 0], [w for w in whole if w[1:] == (0, 0)]]

    def on_device(
        background,
        obs_weight,
        connect,
        live_blocks,
        elem_scale,
        reg_weight,
        iterate,
        residual,
        direction,
        send_nodes,
        send_count,
        ref_stiff,
    ):
        elements = connect.shape[1]
        link = send_nodes.shape[3]
        own_rows = background.shape[1] // LANES
        links = 3 * subs
        rows = -(-(own_rows + links * link // LANES) // 16) * 16
        vmem = pl.BlockSpec(memory_space=pltpu.VMEM)
        smem = pl.BlockSpec(memory_space=pltpu.SMEM)
        partners = sum(len(stage) for stage in stages)
        outs = pl.pallas_call(
            functools.partial(kernel, doms, subs, fields, stages),
            out_shape=[jax.ShapeDtypeStruct((1, elements), F32)] * 3,
            in_specs=[vmem, vmem, vmem, smem, vmem, vmem, vmem, vmem, vmem, vmem, smem, vmem],
            out_specs=[vmem] * 3,
            scratch_shapes=[
                pltpu.VMEM((3, rows, LANES), F32),
                pltpu.VMEM((3 * rows, 2 * LANES), BF16),
                pltpu.VMEM((3 * connect.shape[0], elements), F32),
                pltpu.VMEM((3 * connect.shape[0], elements), F32),
                pltpu.VMEM((6 * rows, LANES), F32),
                pltpu.VMEM((3, own_rows, LANES), F32),
                pltpu.VMEM((max(fields - 1, 1), 3, own_rows, LANES), F32),
                pltpu.VMEM((links, 3, link), F32),
                pltpu.VMEM((links, 3, link), F32),
                pltpu.VMEM((links, 3, link), F32),
                pltpu.VMEM((links, 3, link), F32),
                pltpu.VMEM((links, 3, link), F32),
                pltpu.VMEM((fields, links, 3, link), F32),
                pltpu.VMEM((len(stages) + 1, 8, LANES), F32),
                pltpu.VMEM((partners, 8, LANES), F32),
                pltpu.SemaphoreType.DMA((2, links)),
                pltpu.SemaphoreType.DMA((2, links)),
                pltpu.SemaphoreType.DMA((2, fields, links)),
                pltpu.SemaphoreType.DMA((2, max(fields - 1, 1))),
                pltpu.SemaphoreType.DMA((2, partners)),
            ],
            compiler_params=pltpu.CompilerParams(
                collective_id=0, has_side_effects=True, vmem_limit_bytes=48 * 1024 * 1024
            ),
        )(
            background,
            obs_weight.reshape(own_rows, LANES),
            connect,
            live_blocks,
            elem_scale.reshape(1, elements),
            reg_weight.reshape(1, elements),
            iterate.reshape(1, elements),
            residual.reshape(1, elements),
            direction.reshape(1, elements),
            send_nodes,
            send_count,
            ref_stiff,
        )
        return tuple(x.reshape(elements) for x in outs)

    owned = P(("groups", "dom", "sub"))
    element = P(("groups", "dom", "sub", "field"))
    return jax.shard_map(
        on_device,
        mesh=mesh,
        in_specs=(
            P(None, ("groups", "dom", "sub")),
            owned,
            P(None, ("groups", "dom", "sub", "field")),
            element,
            element,
            element,
            element,
            element,
            element,
            P(("groups", "dom", "sub"), None, None, None),
            P(("groups", "dom", "sub"), None, None),
            P(),
        ),
        out_specs=(element, element, element),
        check_vma=False,
    )
```

```python
import functools

import jax
import jax.numpy as jnp
from jax import lax
from jax.experimental import pallas as pl
from jax.experimental.pallas import tpu as pltpu
from jax.sharding import PartitionSpec as P

BLK = 128
LANES = 128
WIDE = 256
F32 = jnp.float32
BF16 = jnp.bfloat16
MESH = pl.DeviceIdType.MESH


def split(values):
    high = values.astype(BF16)
    return high, (values - high.astype(F32)).astype(BF16)


def hot(index, count):
    rows = lax.broadcasted_iota(jnp.int32, (count, index.shape[1]), 0)
    return jnp.where(rows == (index & (count - 1)), 1.0, 0.0).astype(BF16)


def row_of(index, heights):
    inside = (index >= 0) & (index < heights * WIDE)
    return jnp.where(inside, (index >> 8) + heights * ((index >> 7) & 1), -1)


def picked(table, heights, index):
    rows = 2 * heights
    low = hot(index, LANES)
    wide = jnp.dot(table, jnp.concatenate([low, low], axis=0), preferred_element_type=F32)
    row = row_of(index, heights)
    eight = lax.broadcasted_iota(jnp.int32, (8, index.shape[1]), 0)
    sums = [None] * 3
    for g in range(0, rows, 8):
        mask = eight + g == row
        for c in range(3):
            term = jnp.where(mask, wide[c * rows + g : c * rows + g + 8], 0.0)
            sums[c] = term if sums[c] is None else sums[c] + term
    return sums


def chunked(table, heights, index):
    parts = [picked(table, heights, index[:, e : e + WIDE]) for e in range(0, index.shape[1], WIDE)]
    return [jnp.concatenate([p[c] for p in parts], axis=1) for c in range(3)]


def spread(values, index, heights):
    mask = lax.broadcasted_iota(jnp.int32, (heights, index.shape[1]), 0) == (index >> 8)
    pieces = [split(v) for v in values]
    blocks = []
    for p in range(2):
        for c in range(3):
            piece = jnp.broadcast_to(pieces[c][p].astype(F32), mask.shape)
            blocks.append(jnp.where(mask, piece, 0.0))
    return lax.dot_general(
        jnp.concatenate(blocks, axis=0).astype(BF16),
        hot(index, WIDE),
        (((1,), (1,)), ((), ())),
        preferred_element_type=F32,
    )


def store_table(table, full, rows):
    for c in range(3):
        high, low = split(full[c])
        table[c * rows : (c + 1) * rows, :LANES] = high
        table[c * rows : (c + 1) * rows, LANES:] = low


def kernel(
    doms,
    subs,
    fields,
    stages,
    background,
    obs_weight,
    connect,
    live_blocks,
    elem_scale,
    reg_weight,
    iterate,
    residual,
    direction,
    send_nodes,
    send_count,
    ref_stiff,
    result,
    background_v,
    obs_weight_v,
    connect_v,
    elem_scale_v,
    reg_weight_v,
    iterate_v,
    residual_v,
    direction_v,
    send_nodes_v,
    send_count_v,
    ref_stiff_v,
    own_f,
    ghost_f,
    own_table,
    ghost_table,
    state,
    coupled,
    acc,
    ghost_acc,
    own,
    own_in,
    out_a,
    in_a,
    out_b,
    in_b,
    ret,
    ret_in,
    red,
    red_in,
    sems_in,
    sems_a,
    sems_b,
    sems_r,
    sems_x,
    sems_s,
):
    loads = {}
    given = dict(
        background=(background, background_v),
        send_nodes=(send_nodes, send_nodes_v),
        send_count=(send_count, send_count_v),
        connect=(connect, connect_v),
        direction=(direction, direction_v),
        elem_scale=(elem_scale, elem_scale_v),
        ref_stiff=(ref_stiff, ref_stiff_v),
        obs_weight=(obs_weight, obs_weight_v),
        reg_weight=(reg_weight, reg_weight_v),
        residual=(residual, residual_v),
        iterate=(iterate, iterate_v),
    )
    for i, (name, (source, target)) in enumerate(given.items()):
        loads[name] = pltpu.make_async_copy(source, target, sems_in.at[i])
        loads[name].start()
    background, obs_weight, connect = background_v, obs_weight_v, connect_v
    elem_scale, reg_weight, iterate, residual = elem_scale_v, reg_weight_v, iterate_v, residual_v
    direction, send_nodes, send_count, ref_stiff = direction_v, send_nodes_v, send_count_v, ref_stiff_v

    def arrive(*names):
        for name in names:
            loads[name].wait()

    d, s, f = (lax.axis_index(a) for a in ("dom", "sub", "field"))
    elements = connect.shape[1]
    link = send_nodes.shape[3]
    own_high = own_f.shape[1] // 2
    ghost_high = ghost_f.shape[1] // 2
    owned = own_high * WIDE
    per_link = link // WIDE
    links = [(o, t) for o in range(3) for t in range(subs) if (o, t) != (1, 0)]

    def at(dd, ds, df):
        return {
            "dom": lax.rem(d + dd + doms, doms),
            "sub": lax.rem(s + ds, subs),
            "field": lax.rem(f + df, fields),
        }

    def when(o, step):
        if o == 0:
            pl.when(d > 0)(step)
        elif o == 2:
            pl.when(d < doms - 1)(step)
        else:
            step()

    greeted = {(dd % doms, ds, df) for dd in (-1, 0, 1) for ds in range(subs) for df in range(fields)}
    for stage in stages:
        greeted |= set(stage)
    greeted = sorted(greeted - {(0, 0, 0)})

    in_a[...] = jnp.zeros_like(in_a)
    in_b[...] = jnp.zeros_like(in_b)
    ret_in[...] = jnp.zeros_like(ret_in)
    barrier = pltpu.get_barrier_semaphore()
    for offset in greeted:
        pl.semaphore_signal(barrier, inc=1, device_id=at(*offset), device_id_type=MESH)

    ghost_f[...] = jnp.zeros_like(ghost_f)
    arrive("background", "send_nodes", "send_count")
    for h in range(own_high):
        for half in range(2):
            r = (2 * h + half) * LANES
            own_f[:, half * own_high + h, :] = background[:, r : r + LANES]
    store_table(own_table, own_f, 2 * own_high)

    def outbound(out):
        for o in range(3):
            for t in range(subs):
                index = send_nodes[0, o, t : t + 1, :]
                slot = lax.broadcasted_iota(jnp.int32, index.shape, 1)
                open_slot = jnp.where(slot < send_count[0, t, o], 1.0, 0.0)
                for c, wide in enumerate(picked(own_table[...], own_high, index)):
                    out[o * subs + t, c : c + 1, :] = open_slot * jnp.sum(wide, axis=0, keepdims=True)

    def ghost_copy(o, t, out, landing, sems):
        return pltpu.make_async_remote_copy(
            src_ref=out.at[o * subs + lax.rem(s + t, subs)],
            dst_ref=landing.at[(2 - o) * subs + s],
            send_sem=sems.at[0, o * subs + t],
            recv_sem=sems.at[1, (2 - o) * subs + (subs - t) % subs],
            device_id=at(o - 1, t, 0),
            device_id_type=MESH,
        )

    def ghost_arrival(o, t, out, landing, sems):
        return pltpu.make_async_remote_copy(
            src_ref=out.at[o * subs + lax.rem(s + t, subs)],
            dst_ref=landing.at[o * subs + lax.rem(s + t, subs)],
            send_sem=sems.at[0, o * subs + t],
            recv_sem=sems.at[1, o * subs + t],
            device_id=at(o - 1, t, 0),
            device_id_type=MESH,
        )

    def exchange_start(out, landing, sems):
        for o, t in links:
            when(o, lambda o=o, t=t: ghost_copy(o, t, out, landing, sems).start())

    def exchange_end(out, landing, sems):
        for o, t in links:
            when(o, lambda o=o, t=t: ghost_arrival(o, t, out, landing, sems).wait_recv())

    def ghosts_in(landing):
        for q in range(3 * subs):
            for h in range(per_link):
                for half in range(2):
                    e = (2 * h + half) * LANES
                    ghost_f[:, half * ghost_high + q * per_link + h, :] = landing[q, :, e : e + LANES]
        store_table(ghost_table, ghost_f, 2 * ghost_high)

    outbound(out_a)
    pl.semaphore_wait(barrier, len(greeted))
    exchange_start(out_a, in_a, sems_a)
    arrive("connect", "direction", "elem_scale", "ref_stiff", "obs_weight")
    arrive("reg_weight", "residual", "iterate")

    element = lax.broadcasted_iota(jnp.int32, (1, elements), 1)
    live = jnp.where(element < BLK * live_blocks[0], 1.0, 0.0)
    search = live * direction[...]
    remain = live * residual[...]
    guess = live * iterate[...]
    nodes = connect.shape[0]

    def pull(k, carry):
        index = connect[pl.ds(k, 1), :]
        for c, wide in enumerate(chunked(own_table[...], own_high, index)):
            state[pl.ds(c * nodes + k, 1), :] = jnp.sum(wide, axis=0, keepdims=True)
        return carry

    def pull_ghosts(k, carry):
        index = connect[pl.ds(k, 1), :] - owned
        for c, wide in enumerate(chunked(ghost_table[...], ghost_high, index)):
            state[pl.ds(c * nodes + k, 1), :] += jnp.sum(wide, axis=0, keepdims=True)
        return carry

    lax.fori_loop(0, nodes, pull, 0)
    exchange_end(out_a, in_a, sems_a)
    ghosts_in(in_a)
    lax.fori_loop(0, nodes, pull_ghosts, 0)
    coupled[...] = (live * elem_scale[...]) * jnp.dot(
        ref_stiff[...], state[...], precision=lax.Precision.HIGHEST, preferred_element_type=F32
    )

    acc[...] = jnp.zeros_like(acc)
    ghost_acc[...] = jnp.zeros_like(ghost_acc)

    def push_ghosts(k, carry):
        index = connect[pl.ds(k, 1), :] - owned
        terms = [search * coupled[pl.ds(c * nodes + k, 1), :] for c in range(3)]
        ghost_acc[...] += spread(terms, index, ghost_high)
        return carry

    def push(k, carry):
        index = connect[pl.ds(k, 1), :]
        terms = [search * coupled[pl.ds(c * nodes + k, 1), :] for c in range(3)]
        acc[...] += spread(terms, index, own_high)
        return carry

    lax.fori_loop(0, nodes, push_ghosts, 0)
    for c in range(3):
        total = ghost_acc[c * ghost_high : (c + 1) * ghost_high, :]
        total = total + ghost_acc[(3 + c) * ghost_high : (4 + c) * ghost_high, :]
        for q in range(3 * subs):
            for h in range(per_link):
                r = q * per_link + h
                ret[q, c : c + 1, h * WIDE : (h + 1) * WIDE] = total[r : r + 1]

    def ret_copy(o, t, g):
        return pltpu.make_async_remote_copy(
            src_ref=ret.at[o * subs + lax.rem(s + t, subs)],
            dst_ref=ret_in.at[g, (2 - o) * subs + s],
            send_sem=sems_r.at[0, g, o * subs + t],
            recv_sem=sems_r.at[1, g, (2 - o) * subs + (subs - t) % subs],
            device_id=at(o - 1, t, g),
            device_id_type=MESH,
        )

    def ret_arrival(o, t, g):
        return pltpu.make_async_remote_copy(
            src_ref=ret.at[o * subs + lax.rem(s + t, subs)],
            dst_ref=ret_in.at[g, o * subs + lax.rem(s + t, subs)],
            send_sem=sems_r.at[0, g, o * subs + t],
            recv_sem=sems_r.at[1, g, o * subs + t],
            device_id=at(o - 1, t, g),
            device_id_type=MESH,
        )

    def own_copy(g):
        return pltpu.make_async_remote_copy(
            src_ref=own,
            dst_ref=own_in.at[g - 1],
            send_sem=sems_x.at[0, g - 1],
            recv_sem=sems_x.at[1, g - 1],
            device_id=at(0, 0, g),
            device_id_type=MESH,
        )

    for o, t in links:
        for g in range(fields):
            when(o, lambda o=o, t=t, g=g: ret_copy(o, t, g).start())
    lax.fori_loop(0, nodes, push, 0)
    for c in range(3):
        own[c] = acc[c * own_high : (c + 1) * own_high, :] + acc[(3 + c) * own_high : (4 + c) * own_high, :]
    for g in range(1, fields):
        own_copy(g).start()
    for o, t in links:
        for g in range(fields):
            when(o, lambda o=o, t=t, g=g: ret_arrival(o, t, g).wait_recv())
    landed = None
    for o in range(3):
        for t in range(subs):
            q = o * subs + t
            index = send_nodes[0, o, t : t + 1, :]
            slot = lax.broadcasted_iota(jnp.int32, index.shape, 1)
            open_slot = jnp.where(slot < send_count[0, t, o], 1.0, 0.0)
            sums = ret_in[0, q]
            for g in range(1, fields):
                sums = sums + ret_in[g, q]
            part = spread([open_slot * sums[c : c + 1] for c in range(3)], index, own_high)
            landed = part if landed is None else landed + part
    for g in range(1, fields):
        own_copy(g).wait_recv()
    for c in range(3):
        assembled = own[c]
        for g in range(1, fields):
            assembled = assembled + own_in[g - 1, c]
        assembled = assembled + landed[c * own_high : (c + 1) * own_high]
        assembled = assembled + landed[(3 + c) * own_high : (4 + c) * own_high]
        for half in range(2):
            weight = obs_weight[pl.ds(half, own_high, stride=2), :]
            part = assembled[:, half * LANES : (half + 1) * LANES]
            own_f[c, half * own_high : (half + 1) * own_high, :] = weight * part

    store_table(own_table, own_f, 2 * own_high)
    outbound(out_b)
    exchange_start(out_b, in_b, sems_b)

    def back(table, heights, base):
        def step(k, total):
            index = connect[pl.ds(k, 1), :] - base
            for c, wide in enumerate(chunked(table[...], heights, index)):
                total = total + coupled[pl.ds(c * nodes + k, 1), :] * wide
            return total

        return step

    hess8 = lax.fori_loop(0, nodes, back(own_table, own_high, 0), jnp.zeros((8, elements), F32))
    exchange_end(out_b, in_b, sems_b)
    ghosts_in(in_b)
    hess8 = lax.fori_loop(0, nodes, back(ghost_table, ghost_high, owned), hess8)
    hess = jnp.sum(hess8, axis=0, keepdims=True) + reg_weight[...] * search

    def lane_sums(values):
        total = values[:, :LANES]
        for e in range(LANES, elements, LANES):
            total = total + values[:, e : e + LANES]
        return total

    red[0] = jnp.concatenate(
        [lane_sums(v) for v in (remain * remain, search * hess, remain * hess, hess * hess)]
        + [jnp.zeros((4, LANES), F32)],
        axis=0,
    )
    first = 0
    for n, stage in enumerate(stages):

        def red_copy(i, offset, n=n, first=first):
            return pltpu.make_async_remote_copy(
                src_ref=red.at[n],
                dst_ref=red_in.at[first + i],
                send_sem=sems_s.at[0, first + i],
                recv_sem=sems_s.at[1, first + i],
                device_id=at(*offset),
                device_id_type=MESH,
            )

        for i, offset in enumerate(stage):
            red_copy(i, offset).start()
        total = red[n]
        for i, offset in enumerate(stage):
            red_copy(i, offset).wait_recv()
            total = total + red_in[first + i]
        for i, offset in enumerate(stage):
            red_copy(i, offset).wait_send()
        red[n + 1] = total
        first += len(stage)
    sums = jnp.sum(red[len(stages)], axis=1, keepdims=True)
    before, curvature, cross, image = (sums[i : i + 1] for i in range(4))
    step = before / curvature
    after = before - 2.0 * step * cross + step * step * image
    remain_next = remain - step * hess
    result[0] = guess + step * search
    result[1] = remain_next
    result[2] = remain_next + (after / before) * search
    for out, landing, sems in ((out_a, in_a, sems_a), (out_b, in_b, sems_b)):
        for o, t in links:
            when(
                o,
                lambda o=o, t=t, out=out, landing=landing, sems=sems: ghost_copy(
                    o, t, out, landing, sems
                ).wait_send(),
            )
    for o, t in links:
        for g in range(fields):
            when(o, lambda o=o, t=t, g=g: ret_copy(o, t, g).wait_send())
    for g in range(1, fields):
        own_copy(g).wait_send()


def hand_out(result, iterate_next, residual_next, direction_next, sems):
    outs = (iterate_next, residual_next, direction_next)
    copies = [pltpu.make_async_copy(result.at[i], outs[i], sems.at[i]) for i in range(3)]
    for copy in copies:
        copy.start()
    for copy in copies:
        copy.wait()


def solution(mesh):
    doms, subs, fields = (mesh.shape[a] for a in ("dom", "sub", "field"))
    whole = [(a, b, c) for a in range(doms) for b in range(subs) for c in range(fields)]
    whole = whole[1:]
    if len(whole) < 32:
        stages = [whole]
    else:
        stages = [[w for w in whole if w[0] == 0], [w for w in whole if w[1:] == (0, 0)]]

    def on_device(
        background,
        obs_weight,
        connect,
        live_blocks,
        elem_scale,
        reg_weight,
        iterate,
        residual,
        direction,
        send_nodes,
        send_count,
        ref_stiff,
    ):
        elements = connect.shape[1]
        link = send_nodes.shape[3]
        links = 3 * subs
        nodes = connect.shape[0]
        own_high = background.shape[1] // WIDE
        ghost_high = -(-links * link // WIDE // 8) * 8
        vmem = pl.BlockSpec(memory_space=pltpu.VMEM)
        smem = pl.BlockSpec(memory_space=pltpu.SMEM)
        hbm = pl.BlockSpec(memory_space=pltpu.HBM)
        partners = sum(len(stage) for stage in stages)
        row = (1, elements)
        operands = (
            background,
            obs_weight.reshape(-1, LANES),
            connect,
            live_blocks,
            elem_scale.reshape(row),
            reg_weight.reshape(row),
            iterate.reshape(row),
            residual.reshape(row),
            direction.reshape(row),
            send_nodes,
            send_count.transpose(0, 2, 1),
            ref_stiff,
        )
        spaces = [pltpu.VMEM] * 9 + [pltpu.SMEM, pltpu.VMEM]
        result = pl.pallas_call(
            functools.partial(kernel, doms, subs, fields, stages),
            out_shape=jax.ShapeDtypeStruct((3,) + row, F32),
            in_specs=[hbm] * 3 + [smem] + [hbm] * 8,
            out_specs=vmem,
            scratch_shapes=[space(x.shape, x.dtype) for space, x in zip(spaces, operands[:3] + operands[4:])]
            + [
                pltpu.VMEM((3, 2 * own_high, LANES), F32),
                pltpu.VMEM((3, 2 * ghost_high, LANES), F32),
                pltpu.VMEM((6 * own_high, WIDE), BF16),
                pltpu.VMEM((6 * ghost_high, WIDE), BF16),
                pltpu.VMEM((3 * nodes, elements), F32),
                pltpu.VMEM((3 * nodes, elements), F32),
                pltpu.VMEM((6 * own_high, WIDE), F32),
                pltpu.VMEM((6 * ghost_high, WIDE), F32),
                pltpu.VMEM((3, own_high, WIDE), F32),
                pltpu.VMEM((max(fields - 1, 1), 3, own_high, WIDE), F32),
                pltpu.VMEM((links, 3, link), F32),
                pltpu.VMEM((links, 3, link), F32),
                pltpu.VMEM((links, 3, link), F32),
                pltpu.VMEM((links, 3, link), F32),
                pltpu.VMEM((links, 3, link), F32),
                pltpu.VMEM((fields, links, 3, link), F32),
                pltpu.VMEM((len(stages) + 1, 8, LANES), F32),
                pltpu.VMEM((partners, 8, LANES), F32),
                pltpu.SemaphoreType.DMA((11,)),
                pltpu.SemaphoreType.DMA((2, links)),
                pltpu.SemaphoreType.DMA((2, links)),
                pltpu.SemaphoreType.DMA((2, fields, links)),
                pltpu.SemaphoreType.DMA((2, max(fields - 1, 1))),
                pltpu.SemaphoreType.DMA((2, partners)),
            ],
            compiler_params=pltpu.CompilerParams(
                collective_id=0, has_side_effects=True, vmem_limit_bytes=67043328
            ),
        )(*operands)
        outs = pl.pallas_call(
            hand_out,
            out_shape=[jax.ShapeDtypeStruct(row, F32)] * 3,
            in_specs=[vmem],
            out_specs=[hbm] * 3,
            scratch_shapes=[pltpu.SemaphoreType.DMA((3,))],
        )(result)
        return tuple(x.reshape(elements) for x in outs)

    owned = P(("groups", "dom", "sub"))
    element = P(("groups", "dom", "sub", "field"))
    return jax.shard_map(
        on_device,
        mesh=mesh,
        in_specs=(
            P(None, ("groups", "dom", "sub")),
            owned,
            P(None, ("groups", "dom", "sub", "field")),
            element,
            element,
            element,
            element,
            element,
            element,
            P(("groups", "dom", "sub"), None, None, None),
            P(("groups", "dom", "sub"), None, None),
            P(),
        ),
        out_specs=(element, element, element),
        check_vma=False,
    )
```

```python
import functools

import jax
import jax.numpy as jnp
from jax import lax
from jax.experimental import pallas as pl
from jax.experimental.pallas import tpu as pltpu
from jax.sharding import PartitionSpec as P

BLK = 128
LANES = 128
WIDE = 256
F32 = jnp.float32
BF16 = jnp.bfloat16
MESH = pl.DeviceIdType.MESH


def split(values):
    high = values.astype(BF16)
    return high, (values - high.astype(F32)).astype(BF16)


def hot(index, count):
    rows = lax.broadcasted_iota(jnp.int32, (count, index.shape[1]), 0)
    return jnp.where(rows == (index & (count - 1)), 1.0, 0.0).astype(BF16)


def picked(table, rows, index):
    wide = jnp.dot(table, hot(index, LANES), preferred_element_type=F32)
    row = index >> 7
    eight = lax.broadcasted_iota(jnp.int32, (8, index.shape[1]), 0)
    sums = [None] * 3
    for g in range(0, rows, 8):
        mask = eight + g == row
        for c in range(3):
            high, low = c * rows + g, (3 + c) * rows + g
            term = jnp.where(mask, wide[high : high + 8] + wide[low : low + 8], 0.0)
            sums[c] = term if sums[c] is None else sums[c] + term
    return sums


def chunked(table, rows, index):
    parts = [picked(table, rows, index[:, e : e + WIDE]) for e in range(0, index.shape[1], WIDE)]
    return [jnp.concatenate([p[c] for p in parts], axis=1) for c in range(3)]


def spread(values, index, heights):
    mask = lax.broadcasted_iota(jnp.int32, (heights, index.shape[1]), 0) == (index >> 7)
    pieces = [split(v) for v in values]
    blocks = []
    for p in range(2):
        for c in range(3):
            piece = jnp.broadcast_to(pieces[c][p].astype(F32), mask.shape)
            blocks.append(jnp.where(mask, piece, 0.0))
    return lax.dot_general(
        jnp.concatenate(blocks, axis=0).astype(BF16),
        hot(index, LANES),
        (((1,), (1,)), ((), ())),
        preferred_element_type=F32,
    )


def store_table(table, full, rows):
    for c in range(3):
        high, low = split(full[c])
        table[c * rows : (c + 1) * rows, :] = high
        table[(3 + c) * rows : (4 + c) * rows, :] = low


def kernel(
    doms,
    subs,
    fields,
    stages,
    background,
    obs_weight,
    connect,
    live_blocks,
    elem_scale,
    reg_weight,
    iterate,
    residual,
    direction,
    send_nodes,
    send_count,
    ref_stiff,
    result,
    background_v,
    obs_weight_v,
    connect_v,
    elem_scale_v,
    reg_weight_v,
    iterate_v,
    residual_v,
    direction_v,
    send_nodes_v,
    send_count_v,
    ref_stiff_v,
    own_f,
    ghost_f,
    own_table,
    ghost_table,
    state,
    coupled,
    acc,
    ghost_acc,
    own,
    own_in,
    out_a,
    in_a,
    out_b,
    in_b,
    ret,
    ret_in,
    red,
    red_in,
    sems_in,
    sems_a,
    sems_b,
    sems_r,
    sems_x,
    sems_s,
):
    loads = {}
    given = dict(
        background=(background, background_v),
        send_nodes=(send_nodes, send_nodes_v),
        send_count=(send_count, send_count_v),
        connect=(connect, connect_v),
        direction=(direction, direction_v),
        elem_scale=(elem_scale, elem_scale_v),
        ref_stiff=(ref_stiff, ref_stiff_v),
        obs_weight=(obs_weight, obs_weight_v),
        reg_weight=(reg_weight, reg_weight_v),
        residual=(residual, residual_v),
        iterate=(iterate, iterate_v),
    )
    for i, (name, (source, target)) in enumerate(given.items()):
        loads[name] = pltpu.make_async_copy(source, target, sems_in.at[i])
        loads[name].start()
    background, obs_weight, connect = background_v, obs_weight_v, connect_v
    elem_scale, reg_weight, iterate, residual = elem_scale_v, reg_weight_v, iterate_v, residual_v
    direction, send_nodes, send_count, ref_stiff = direction_v, send_nodes_v, send_count_v, ref_stiff_v

    def arrive(*names):
        for name in names:
            loads[name].wait()

    d, s, f = (lax.axis_index(a) for a in ("dom", "sub", "field"))
    elements = connect.shape[1]
    link = send_nodes.shape[3]
    own_high = own_f.shape[1]
    ghost_high = ghost_f.shape[1]
    owned = own_high * LANES
    per_link = link // LANES
    links = [(o, t) for o in range(3) for t in range(subs) if (o, t) != (1, 0)]

    def at(dd, ds, df):
        return {
            "dom": lax.rem(d + dd + doms, doms),
            "sub": lax.rem(s + ds, subs),
            "field": lax.rem(f + df, fields),
        }

    def when(o, step):
        if o == 0:
            pl.when(d > 0)(step)
        elif o == 2:
            pl.when(d < doms - 1)(step)
        else:
            step()

    greeted = {(dd % doms, ds, df) for dd in (-1, 0, 1) for ds in range(subs) for df in range(fields)}
    for stage in stages:
        greeted |= set(stage)
    greeted = sorted(greeted - {(0, 0, 0)})

    in_a[...] = jnp.zeros_like(in_a)
    in_b[...] = jnp.zeros_like(in_b)
    ret_in[...] = jnp.zeros_like(ret_in)
    barrier = pltpu.get_barrier_semaphore()
    for offset in greeted:
        pl.semaphore_signal(barrier, inc=1, device_id=at(*offset), device_id_type=MESH)

    ghost_f[...] = jnp.zeros_like(ghost_f)
    arrive("background", "send_nodes", "send_count")
    for h in range(own_high):
        own_f[:, h, :] = background[:, h * LANES : (h + 1) * LANES]
    store_table(own_table, own_f, own_high)

    def link_index(o, t):
        other = lax.rem(s + t, subs)
        index = send_nodes[0, o, pl.ds(other, 1), :]
        slot = lax.broadcasted_iota(jnp.int32, index.shape, 1)
        return index, jnp.where(slot < send_count[0, other, o], 1.0, 0.0), o * subs + other

    def outbound(out):
        for o, t in links:
            index, open_slot, q = link_index(o, t)
            for c, wide in enumerate(picked(own_table[...], own_high, index)):
                out[q, c : c + 1, :] = open_slot * jnp.sum(wide, axis=0, keepdims=True)

    def ghost_copy(o, t, out, landing, sems):
        return pltpu.make_async_remote_copy(
            src_ref=out.at[o * subs + lax.rem(s + t, subs)],
            dst_ref=landing.at[(2 - o) * subs + s],
            send_sem=sems.at[0, o * subs + t],
            recv_sem=sems.at[1, (2 - o) * subs + (subs - t) % subs],
            device_id=at(o - 1, t, 0),
            device_id_type=MESH,
        )

    def ghost_arrival(o, t, out, landing, sems):
        return pltpu.make_async_remote_copy(
            src_ref=out.at[o * subs + lax.rem(s + t, subs)],
            dst_ref=landing.at[o * subs + lax.rem(s + t, subs)],
            send_sem=sems.at[0, o * subs + t],
            recv_sem=sems.at[1, o * subs + t],
            device_id=at(o - 1, t, 0),
            device_id_type=MESH,
        )

    def exchange_start(out, landing, sems):
        for o, t in links:
            when(o, lambda o=o, t=t: ghost_copy(o, t, out, landing, sems).start())

    def exchange_end(out, landing, sems):
        for o, t in links:
            when(o, lambda o=o, t=t: ghost_arrival(o, t, out, landing, sems).wait_recv())

    def ghosts_in(landing):
        for q in range(3 * subs):
            for h in range(per_link):
                ghost_f[:, q * per_link + h, :] = landing[q, :, h * LANES : (h + 1) * LANES]
        store_table(ghost_table, ghost_f, ghost_high)

    outbound(out_a)
    pl.semaphore_wait(barrier, len(greeted))
    exchange_start(out_a, in_a, sems_a)
    arrive("connect", "direction", "elem_scale", "ref_stiff", "obs_weight")
    arrive("reg_weight", "residual", "iterate")

    element = lax.broadcasted_iota(jnp.int32, (1, elements), 1)
    live = jnp.where(element < BLK * live_blocks[0], 1.0, 0.0)
    search = live * direction[...]
    remain = live * residual[...]
    guess = live * iterate[...]
    nodes = connect.shape[0]

    def pull(k, carry):
        index = connect[pl.ds(k, 1), :]
        for c, wide in enumerate(chunked(own_table[...], own_high, index)):
            state[pl.ds(c * nodes + k, 1), :] = jnp.sum(wide, axis=0, keepdims=True)
        return carry

    def pull_ghosts(k, carry):
        index = connect[pl.ds(k, 1), :] - owned
        for c, wide in enumerate(chunked(ghost_table[...], ghost_high, index)):
            state[pl.ds(c * nodes + k, 1), :] += jnp.sum(wide, axis=0, keepdims=True)
        return carry

    lax.fori_loop(0, nodes, pull, 0)
    exchange_end(out_a, in_a, sems_a)
    ghosts_in(in_a)
    lax.fori_loop(0, nodes, pull_ghosts, 0)
    coupled[...] = (live * elem_scale[...]) * jnp.dot(
        ref_stiff[...], state[...], precision=lax.Precision.HIGHEST, preferred_element_type=F32
    )

    acc[...] = jnp.zeros_like(acc)
    ghost_acc[...] = jnp.zeros_like(ghost_acc)

    def push_ghosts(k, carry):
        index = connect[pl.ds(k, 1), :] - owned
        terms = [search * coupled[pl.ds(c * nodes + k, 1), :] for c in range(3)]
        ghost_acc[...] += spread(terms, index, ghost_high)
        return carry

    def push(k, carry):
        index = connect[pl.ds(k, 1), :]
        terms = [search * coupled[pl.ds(c * nodes + k, 1), :] for c in range(3)]
        acc[...] += spread(terms, index, own_high)
        return carry

    lax.fori_loop(0, nodes, push_ghosts, 0)
    for c in range(3):
        total = ghost_acc[c * ghost_high : (c + 1) * ghost_high, :]
        total = total + ghost_acc[(3 + c) * ghost_high : (4 + c) * ghost_high, :]
        for q in range(3 * subs):
            for h in range(per_link):
                r = q * per_link + h
                ret[q, c : c + 1, h * LANES : (h + 1) * LANES] = total[r : r + 1]

    def ret_copy(o, t, g):
        return pltpu.make_async_remote_copy(
            src_ref=ret.at[o * subs + lax.rem(s + t, subs)],
            dst_ref=ret_in.at[g, (2 - o) * subs + s],
            send_sem=sems_r.at[0, g, o * subs + t],
            recv_sem=sems_r.at[1, g, (2 - o) * subs + (subs - t) % subs],
            device_id=at(o - 1, t, g),
            device_id_type=MESH,
        )

    def ret_arrival(o, t, g):
        return pltpu.make_async_remote_copy(
            src_ref=ret.at[o * subs + lax.rem(s + t, subs)],
            dst_ref=ret_in.at[g, o * subs + lax.rem(s + t, subs)],
            send_sem=sems_r.at[0, g, o * subs + t],
            recv_sem=sems_r.at[1, g, o * subs + t],
            device_id=at(o - 1, t, g),
            device_id_type=MESH,
        )

    def own_copy(g):
        return pltpu.make_async_remote_copy(
            src_ref=own,
            dst_ref=own_in.at[g - 1],
            send_sem=sems_x.at[0, g - 1],
            recv_sem=sems_x.at[1, g - 1],
            device_id=at(0, 0, g),
            device_id_type=MESH,
        )

    for o, t in links:
        for g in range(fields):
            when(o, lambda o=o, t=t, g=g: ret_copy(o, t, g).start())
    lax.fori_loop(0, nodes, push, 0)
    for c in range(3):
        own[c] = acc[c * own_high : (c + 1) * own_high, :] + acc[(3 + c) * own_high : (4 + c) * own_high, :]
    for g in range(1, fields):
        own_copy(g).start()
    for o, t in links:
        for g in range(fields):
            when(o, lambda o=o, t=t, g=g: ret_arrival(o, t, g).wait_recv())
    landed = None
    for o, t in links:
        index, open_slot, q = link_index(o, t)
        sums = ret_in[0, q]
        for g in range(1, fields):
            sums = sums + ret_in[g, q]
        part = spread([open_slot * sums[c : c + 1] for c in range(3)], index, own_high)
        landed = part if landed is None else landed + part
    for g in range(1, fields):
        own_copy(g).wait_recv()
    for c in range(3):
        assembled = own[c]
        for g in range(1, fields):
            assembled = assembled + own_in[g - 1, c]
        assembled = assembled + landed[c * own_high : (c + 1) * own_high]
        assembled = assembled + landed[(3 + c) * own_high : (4 + c) * own_high]
        own_f[c] = obs_weight[...] * assembled

    store_table(own_table, own_f, own_high)
    outbound(out_b)
    exchange_start(out_b, in_b, sems_b)

    def back(table, heights, base):
        def step(k, total):
            index = connect[pl.ds(k, 1), :] - base
            for c, wide in enumerate(chunked(table[...], heights, index)):
                total = total + coupled[pl.ds(c * nodes + k, 1), :] * wide
            return total

        return step

    hess8 = lax.fori_loop(0, nodes, back(own_table, own_high, 0), jnp.zeros((8, elements), F32))
    exchange_end(out_b, in_b, sems_b)
    ghosts_in(in_b)
    hess8 = lax.fori_loop(0, nodes, back(ghost_table, ghost_high, owned), hess8)
    hess = jnp.sum(hess8, axis=0, keepdims=True) + reg_weight[...] * search

    def lane_sums(values):
        total = values[:, :LANES]
        for e in range(LANES, elements, LANES):
            total = total + values[:, e : e + LANES]
        return total

    red[0] = jnp.concatenate(
        [lane_sums(v) for v in (remain * remain, search * hess, remain * hess, hess * hess)]
        + [jnp.zeros((4, LANES), F32)],
        axis=0,
    )
    first = 0
    for n, stage in enumerate(stages):

        def red_copy(i, offset, n=n, first=first):
            return pltpu.make_async_remote_copy(
                src_ref=red.at[n],
                dst_ref=red_in.at[first + i],
                send_sem=sems_s.at[0, first + i],
                recv_sem=sems_s.at[1, first + i],
                device_id=at(*offset),
                device_id_type=MESH,
            )

        for i, offset in enumerate(stage):
            red_copy(i, offset).start()
        total = red[n]
        for i, offset in enumerate(stage):
            red_copy(i, offset).wait_recv()
            total = total + red_in[first + i]
        for i, offset in enumerate(stage):
            red_copy(i, offset).wait_send()
        red[n + 1] = total
        first += len(stage)
    sums = jnp.sum(red[len(stages)], axis=1, keepdims=True)
    before, curvature, cross, image = (sums[i : i + 1] for i in range(4))
    step = before / curvature
    after = before - 2.0 * step * cross + step * step * image
    remain_next = remain - step * hess
    result[0] = guess + step * search
    result[1] = remain_next
    result[2] = remain_next + (after / before) * search
    for out, landing, sems in ((out_a, in_a, sems_a), (out_b, in_b, sems_b)):
        for o, t in links:
            when(
                o,
                lambda o=o, t=t, out=out, landing=landing, sems=sems: ghost_copy(
                    o, t, out, landing, sems
                ).wait_send(),
            )
    for o, t in links:
        for g in range(fields):
            when(o, lambda o=o, t=t, g=g: ret_copy(o, t, g).wait_send())
    for g in range(1, fields):
        own_copy(g).wait_send()


def hand_out(result, iterate_next, residual_next, direction_next, sems):
    outs = (iterate_next, residual_next, direction_next)
    copies = [pltpu.make_async_copy(result.at[i], outs[i], sems.at[i]) for i in range(3)]
    for copy in copies:
        copy.start()
    for copy in copies:
        copy.wait()


def solution(mesh):
    doms, subs, fields = (mesh.shape[a] for a in ("dom", "sub", "field"))
    whole = [(a, b, c) for a in range(doms) for b in range(subs) for c in range(fields)]
    whole = whole[1:]
    if len(whole) < 32:
        stages = [whole]
    else:
        stages = [[w for w in whole if w[0] == 0], [w for w in whole if w[1:] == (0, 0)]]

    def on_device(
        background,
        obs_weight,
        connect,
        live_blocks,
        elem_scale,
        reg_weight,
        iterate,
        residual,
        direction,
        send_nodes,
        send_count,
        ref_stiff,
    ):
        elements = connect.shape[1]
        link = send_nodes.shape[3]
        links = 3 * subs
        nodes = connect.shape[0]
        own_high = background.shape[1] // LANES
        ghost_high = -(-links * link // LANES // 16) * 16
        vmem = pl.BlockSpec(memory_space=pltpu.VMEM)
        smem = pl.BlockSpec(memory_space=pltpu.SMEM)
        hbm = pl.BlockSpec(memory_space=pltpu.HBM)
        partners = sum(len(stage) for stage in stages)
        row = (1, elements)
        operands = (
            background,
            obs_weight.reshape(-1, LANES),
            connect,
            live_blocks,
            elem_scale.reshape(row),
            reg_weight.reshape(row),
            iterate.reshape(row),
            residual.reshape(row),
            direction.reshape(row),
            send_nodes,
            send_count.transpose(0, 2, 1),
            ref_stiff,
        )
        spaces = [pltpu.VMEM] * 9 + [pltpu.SMEM, pltpu.VMEM]
        result = pl.pallas_call(
            functools.partial(kernel, doms, subs, fields, stages),
            out_shape=jax.ShapeDtypeStruct((3,) + row, F32),
            in_specs=[hbm] * 3 + [smem] + [hbm] * 8,
            out_specs=vmem,
            scratch_shapes=[space(x.shape, x.dtype) for space, x in zip(spaces, operands[:3] + operands[4:])]
            + [
                pltpu.VMEM((3, own_high, LANES), F32),
                pltpu.VMEM((3, ghost_high, LANES), F32),
                pltpu.VMEM((6 * own_high, LANES), BF16),
                pltpu.VMEM((6 * ghost_high, LANES), BF16),
                pltpu.VMEM((3 * nodes, elements), F32),
                pltpu.VMEM((3 * nodes, elements), F32),
                pltpu.VMEM((6 * own_high, LANES), F32),
                pltpu.VMEM((6 * ghost_high, LANES), F32),
                pltpu.VMEM((3, own_high, LANES), F32),
                pltpu.VMEM((max(fields - 1, 1), 3, own_high, LANES), F32),
                pltpu.VMEM((links, 3, link), F32),
                pltpu.VMEM((links, 3, link), F32),
                pltpu.VMEM((links, 3, link), F32),
                pltpu.VMEM((links, 3, link), F32),
                pltpu.VMEM((links, 3, link), F32),
                pltpu.VMEM((fields, links, 3, link), F32),
                pltpu.VMEM((len(stages) + 1, 8, LANES), F32),
                pltpu.VMEM((partners, 8, LANES), F32),
                pltpu.SemaphoreType.DMA((11,)),
                pltpu.SemaphoreType.DMA((2, links)),
                pltpu.SemaphoreType.DMA((2, links)),
                pltpu.SemaphoreType.DMA((2, fields, links)),
                pltpu.SemaphoreType.DMA((2, max(fields - 1, 1))),
                pltpu.SemaphoreType.DMA((2, partners)),
            ],
            compiler_params=pltpu.CompilerParams(
                collective_id=0, has_side_effects=True, vmem_limit_bytes=67043328
            ),
        )(*operands)
        outs = pl.pallas_call(
            hand_out,
            out_shape=[jax.ShapeDtypeStruct(row, F32)] * 3,
            in_specs=[vmem],
            out_specs=[hbm] * 3,
            scratch_shapes=[pltpu.SemaphoreType.DMA((3,))],
        )(result)
        return tuple(x.reshape(elements) for x in outs)

    owned = P(("groups", "dom", "sub"))
    element = P(("groups", "dom", "sub", "field"))
    return jax.shard_map(
        on_device,
        mesh=mesh,
        in_specs=(
            P(None, ("groups", "dom", "sub")),
            owned,
            P(None, ("groups", "dom", "sub", "field")),
            element,
            element,
            element,
            element,
            element,
            element,
            P(("groups", "dom", "sub"), None, None, None),
            P(("groups", "dom", "sub"), None, None),
            P(),
        ),
        out_specs=(element, element, element),
        check_vma=False,
    )
```

```python
import functools

import jax
import jax.numpy as jnp
from jax import lax
from jax.experimental import pallas as pl
from jax.experimental.pallas import tpu as pltpu
from jax.sharding import PartitionSpec as P

BLK = 128
UNROLL = 2
LANES = 128
WIDE = 256
F32 = jnp.float32
BF16 = jnp.bfloat16
MESH = pl.DeviceIdType.MESH


def split(values):
    high = values.astype(BF16)
    return high, (values - high.astype(F32)).astype(BF16)


def hot(index, count):
    rows = lax.broadcasted_iota(jnp.int32, (count, index.shape[1]), 0)
    return jnp.where(rows == (index & (count - 1)), 1.0, 0.0).astype(BF16)


def picked(table, rows, index):
    wide = jnp.dot(table, hot(index, LANES), preferred_element_type=F32)
    row = index >> 7
    eight = lax.broadcasted_iota(jnp.int32, (8, index.shape[1]), 0)
    sums = [None] * 3
    for g in range(0, rows, 8):
        mask = eight + g == row
        for c in range(3):
            high, low = c * rows + g, (3 + c) * rows + g
            term = jnp.where(mask, wide[high : high + 8] + wide[low : low + 8], 0.0)
            sums[c] = term if sums[c] is None else sums[c] + term
    return sums


def chunked(table, rows, index):
    parts = [picked(table, rows, index[:, e : e + WIDE]) for e in range(0, index.shape[1], WIDE)]
    return [jnp.concatenate([p[c] for p in parts], axis=1) for c in range(3)]


def spread(values, index, heights):
    row = jnp.broadcast_to(index >> 7, (16, index.shape[1])).astype(jnp.int16)
    place = lax.broadcasted_iota(jnp.int32, (16, index.shape[1]), 0).astype(jnp.int16)
    pieces = [split(jnp.broadcast_to(v, (16, v.shape[1]))) for v in values]
    zero = jnp.zeros(row.shape, BF16)
    blocks = []
    for p in range(2):
        for c in range(3):
            for g in range(0, heights, 16):
                blocks.append(jnp.where(place + jnp.int16(g) == row, pieces[c][p], zero))
    return lax.dot_general(
        jnp.concatenate(blocks, axis=0),
        hot(index, LANES),
        (((1,), (1,)), ((), ())),
        preferred_element_type=F32,
    )


def each(count, step, carry):
    by = next(u for u in (UNROLL, 1) if count % u == 0)

    def trip(i, carry):
        for j in range(by):
            carry = step(i * by + j, carry)
        return carry

    return lax.fori_loop(0, count // by, trip, carry)


def store_table(table, full, rows):
    for c in range(3):
        high, low = split(full[c])
        table[c * rows : (c + 1) * rows, :] = high
        table[(3 + c) * rows : (4 + c) * rows, :] = low


def kernel(
    doms,
    subs,
    fields,
    stages,
    background,
    obs_weight,
    connect,
    live_blocks,
    elem_scale,
    reg_weight,
    iterate,
    residual,
    direction,
    send_nodes,
    send_count,
    ref_stiff,
    result,
    background_v,
    obs_weight_v,
    connect_v,
    elem_scale_v,
    reg_weight_v,
    iterate_v,
    residual_v,
    direction_v,
    send_nodes_v,
    send_count_v,
    ref_stiff_v,
    own_f,
    ghost_f,
    own_table,
    ghost_table,
    state,
    coupled,
    acc,
    ghost_acc,
    own,
    own_in,
    out_a,
    in_a,
    out_b,
    in_b,
    ret,
    ret_in,
    red,
    red_in,
    sems_in,
    sems_a,
    sems_b,
    sems_r,
    sems_x,
    sems_s,
):
    loads = {}
    given = dict(
        background=(background, background_v),
        send_nodes=(send_nodes, send_nodes_v),
        send_count=(send_count, send_count_v),
        connect=(connect, connect_v),
        direction=(direction, direction_v),
        elem_scale=(elem_scale, elem_scale_v),
        ref_stiff=(ref_stiff, ref_stiff_v),
        obs_weight=(obs_weight, obs_weight_v),
        reg_weight=(reg_weight, reg_weight_v),
        residual=(residual, residual_v),
        iterate=(iterate, iterate_v),
    )
    for i, (name, (source, target)) in enumerate(given.items()):
        loads[name] = pltpu.make_async_copy(source, target, sems_in.at[i])
        loads[name].start()
    background, obs_weight, connect = background_v, obs_weight_v, connect_v
    elem_scale, reg_weight, iterate, residual = elem_scale_v, reg_weight_v, iterate_v, residual_v
    direction, send_nodes, send_count, ref_stiff = direction_v, send_nodes_v, send_count_v, ref_stiff_v

    def arrive(*names):
        for name in names:
            loads[name].wait()

    d, s, f = (lax.axis_index(a) for a in ("dom", "sub", "field"))
    elements = connect.shape[1]
    link = send_nodes.shape[3]
    own_high = own_f.shape[1]
    ghost_high = ghost_f.shape[1]
    owned = own_high * LANES
    per_link = link // LANES
    links = [(o, t) for o in range(3) for t in range(subs) if (o, t) != (1, 0)]

    def at(dd, ds, df):
        return {
            "dom": lax.rem(d + dd + doms, doms),
            "sub": lax.rem(s + ds, subs),
            "field": lax.rem(f + df, fields),
        }

    def when(o, step):
        if o == 0:
            pl.when(d > 0)(step)
        elif o == 2:
            pl.when(d < doms - 1)(step)
        else:
            step()

    greeted = {(dd % doms, ds, df) for dd in (-1, 0, 1) for ds in range(subs) for df in range(fields)}
    for stage in stages:
        greeted |= set(stage)
    greeted = sorted(greeted - {(0, 0, 0)})

    in_a[...] = jnp.zeros_like(in_a)
    in_b[...] = jnp.zeros_like(in_b)
    ret_in[...] = jnp.zeros_like(ret_in)
    barrier = pltpu.get_barrier_semaphore()
    for offset in greeted:
        pl.semaphore_signal(barrier, inc=1, device_id=at(*offset), device_id_type=MESH)

    ghost_f[...] = jnp.zeros_like(ghost_f)
    arrive("background", "send_nodes", "send_count")
    for h in range(own_high):
        own_f[:, h, :] = background[:, h * LANES : (h + 1) * LANES]
    store_table(own_table, own_f, own_high)

    def link_index(o, t):
        other = lax.rem(s + t, subs)
        index = send_nodes[0, o, pl.ds(other, 1), :]
        slot = lax.broadcasted_iota(jnp.int32, index.shape, 1)
        return index, jnp.where(slot < send_count[0, other, o], 1.0, 0.0), o * subs + other

    def outbound(out):
        for o, t in links:
            index, open_slot, q = link_index(o, t)
            for c, wide in enumerate(picked(own_table[...], own_high, index)):
                out[q, c : c + 1, :] = open_slot * jnp.sum(wide, axis=0, keepdims=True)

    def ghost_copy(o, t, out, landing, sems):
        return pltpu.make_async_remote_copy(
            src_ref=out.at[o * subs + lax.rem(s + t, subs)],
            dst_ref=landing.at[(2 - o) * subs + s],
            send_sem=sems.at[0, o * subs + t],
            recv_sem=sems.at[1, (2 - o) * subs + (subs - t) % subs],
            device_id=at(o - 1, t, 0),
            device_id_type=MESH,
        )

    def ghost_arrival(o, t, out, landing, sems):
        return pltpu.make_async_remote_copy(
            src_ref=out.at[o * subs + lax.rem(s + t, subs)],
            dst_ref=landing.at[o * subs + lax.rem(s + t, subs)],
            send_sem=sems.at[0, o * subs + t],
            recv_sem=sems.at[1, o * subs + t],
            device_id=at(o - 1, t, 0),
            device_id_type=MESH,
        )

    def exchange_start(out, landing, sems):
        for o, t in links:
            when(o, lambda o=o, t=t: ghost_copy(o, t, out, landing, sems).start())

    def exchange_end(out, landing, sems):
        for o, t in links:
            when(o, lambda o=o, t=t: ghost_arrival(o, t, out, landing, sems).wait_recv())

    def ghosts_in(landing):
        for q in range(3 * subs):
            for h in range(per_link):
                ghost_f[:, q * per_link + h, :] = landing[q, :, h * LANES : (h + 1) * LANES]
        store_table(ghost_table, ghost_f, ghost_high)

    outbound(out_a)
    pl.semaphore_wait(barrier, len(greeted))
    exchange_start(out_a, in_a, sems_a)
    arrive("connect", "direction", "elem_scale", "ref_stiff", "obs_weight")
    arrive("reg_weight", "residual", "iterate")

    element = lax.broadcasted_iota(jnp.int32, (1, elements), 1)
    live = jnp.where(element < BLK * live_blocks[0], 1.0, 0.0)
    search = live * direction[...]
    remain = live * residual[...]
    guess = live * iterate[...]
    nodes = connect.shape[0]

    def pull(k, carry):
        index = connect[pl.ds(k, 1), :]
        for c, wide in enumerate(chunked(own_table[...], own_high, index)):
            state[pl.ds(c * nodes + k, 1), :] = jnp.sum(wide, axis=0, keepdims=True)
        return carry

    def pull_ghosts(k, carry):
        index = connect[pl.ds(k, 1), :] - owned
        for c, wide in enumerate(chunked(ghost_table[...], ghost_high, index)):
            state[pl.ds(c * nodes + k, 1), :] += jnp.sum(wide, axis=0, keepdims=True)
        return carry

    each(nodes, pull, 0)
    exchange_end(out_a, in_a, sems_a)
    ghosts_in(in_a)
    each(nodes, pull_ghosts, 0)
    coupled[...] = (live * elem_scale[...]) * jnp.dot(
        ref_stiff[...], state[...], precision=lax.Precision.HIGHEST, preferred_element_type=F32
    )

    acc[...] = jnp.zeros_like(acc)
    ghost_acc[...] = jnp.zeros_like(ghost_acc)

    def push_ghosts(k, carry):
        index = connect[pl.ds(k, 1), :] - owned
        terms = [search * coupled[pl.ds(c * nodes + k, 1), :] for c in range(3)]
        ghost_acc[...] += spread(terms, index, ghost_high)
        return carry

    def push(k, carry):
        index = connect[pl.ds(k, 1), :]
        terms = [search * coupled[pl.ds(c * nodes + k, 1), :] for c in range(3)]
        acc[...] += spread(terms, index, own_high)
        return carry

    each(nodes, push_ghosts, 0)
    for c in range(3):
        total = ghost_acc[c * ghost_high : (c + 1) * ghost_high, :]
        total = total + ghost_acc[(3 + c) * ghost_high : (4 + c) * ghost_high, :]
        for q in range(3 * subs):
            for h in range(per_link):
                r = q * per_link + h
                ret[q, c : c + 1, h * LANES : (h + 1) * LANES] = total[r : r + 1]

    def ret_copy(o, t, g):
        return pltpu.make_async_remote_copy(
            src_ref=ret.at[o * subs + lax.rem(s + t, subs)],
            dst_ref=ret_in.at[g, (2 - o) * subs + s],
            send_sem=sems_r.at[0, g, o * subs + t],
            recv_sem=sems_r.at[1, g, (2 - o) * subs + (subs - t) % subs],
            device_id=at(o - 1, t, g),
            device_id_type=MESH,
        )

    def ret_arrival(o, t, g):
        return pltpu.make_async_remote_copy(
            src_ref=ret.at[o * subs + lax.rem(s + t, subs)],
            dst_ref=ret_in.at[g, o * subs + lax.rem(s + t, subs)],
            send_sem=sems_r.at[0, g, o * subs + t],
            recv_sem=sems_r.at[1, g, o * subs + t],
            device_id=at(o - 1, t, g),
            device_id_type=MESH,
        )

    def own_copy(g):
        return pltpu.make_async_remote_copy(
            src_ref=own,
            dst_ref=own_in.at[g - 1],
            send_sem=sems_x.at[0, g - 1],
            recv_sem=sems_x.at[1, g - 1],
            device_id=at(0, 0, g),
            device_id_type=MESH,
        )

    for o, t in links:
        for g in range(fields):
            when(o, lambda o=o, t=t, g=g: ret_copy(o, t, g).start())
    each(nodes, push, 0)
    for c in range(3):
        own[c] = acc[c * own_high : (c + 1) * own_high, :] + acc[(3 + c) * own_high : (4 + c) * own_high, :]
    for g in range(1, fields):
        own_copy(g).start()
    for o, t in links:
        for g in range(fields):
            when(o, lambda o=o, t=t, g=g: ret_arrival(o, t, g).wait_recv())
    landed = None
    for o, t in links:
        index, open_slot, q = link_index(o, t)
        sums = ret_in[0, q]
        for g in range(1, fields):
            sums = sums + ret_in[g, q]
        part = spread([open_slot * sums[c : c + 1] for c in range(3)], index, own_high)
        landed = part if landed is None else landed + part
    for g in range(1, fields):
        own_copy(g).wait_recv()
    for c in range(3):
        assembled = own[c]
        for g in range(1, fields):
            assembled = assembled + own_in[g - 1, c]
        assembled = assembled + landed[c * own_high : (c + 1) * own_high]
        assembled = assembled + landed[(3 + c) * own_high : (4 + c) * own_high]
        own_f[c] = obs_weight[...] * assembled

    store_table(own_table, own_f, own_high)
    outbound(out_b)
    exchange_start(out_b, in_b, sems_b)

    def back(table, heights, base):
        def step(k, total):
            index = connect[pl.ds(k, 1), :] - base
            for c, wide in enumerate(chunked(table[...], heights, index)):
                total = total + coupled[pl.ds(c * nodes + k, 1), :] * wide
            return total

        return step

    hess8 = each(nodes, back(own_table, own_high, 0), jnp.zeros((8, elements), F32))
    exchange_end(out_b, in_b, sems_b)
    ghosts_in(in_b)
    hess8 = each(nodes, back(ghost_table, ghost_high, owned), hess8)
    hess = jnp.sum(hess8, axis=0, keepdims=True) + reg_weight[...] * search

    def lane_sums(values):
        total = values[:, :LANES]
        for e in range(LANES, elements, LANES):
            total = total + values[:, e : e + LANES]
        return total

    red[0] = jnp.concatenate(
        [lane_sums(v) for v in (remain * remain, search * hess, remain * hess, hess * hess)]
        + [jnp.zeros((4, LANES), F32)],
        axis=0,
    )
    first = 0
    for n, stage in enumerate(stages):

        def red_copy(i, offset, n=n, first=first):
            return pltpu.make_async_remote_copy(
                src_ref=red.at[n],
                dst_ref=red_in.at[first + i],
                send_sem=sems_s.at[0, first + i],
                recv_sem=sems_s.at[1, first + i],
                device_id=at(*offset),
                device_id_type=MESH,
            )

        for i, offset in enumerate(stage):
            red_copy(i, offset).start()
        total = red[n]
        for i, offset in enumerate(stage):
            red_copy(i, offset).wait_recv()
            total = total + red_in[first + i]
        for i, offset in enumerate(stage):
            red_copy(i, offset).wait_send()
        red[n + 1] = total
        first += len(stage)
    sums = jnp.sum(red[len(stages)], axis=1, keepdims=True)
    before, curvature, cross, image = (sums[i : i + 1] for i in range(4))
    step = before / curvature
    after = before - 2.0 * step * cross + step * step * image
    remain_next = remain - step * hess
    result[0] = guess + step * search
    result[1] = remain_next
    result[2] = remain_next + (after / before) * search
    for out, landing, sems in ((out_a, in_a, sems_a), (out_b, in_b, sems_b)):
        for o, t in links:
            when(
                o,
                lambda o=o, t=t, out=out, landing=landing, sems=sems: ghost_copy(
                    o, t, out, landing, sems
                ).wait_send(),
            )
    for o, t in links:
        for g in range(fields):
            when(o, lambda o=o, t=t, g=g: ret_copy(o, t, g).wait_send())
    for g in range(1, fields):
        own_copy(g).wait_send()


def hand_out(result, iterate_next, residual_next, direction_next, sems):
    outs = (iterate_next, residual_next, direction_next)
    copies = [pltpu.make_async_copy(result.at[i], outs[i], sems.at[i]) for i in range(3)]
    for copy in copies:
        copy.start()
    for copy in copies:
        copy.wait()


def solution(mesh):
    doms, subs, fields = (mesh.shape[a] for a in ("dom", "sub", "field"))
    whole = [(a, b, c) for a in range(doms) for b in range(subs) for c in range(fields)]
    whole = whole[1:]
    if len(whole) < 32:
        stages = [whole]
    else:
        stages = [[w for w in whole if w[0] == 0], [w for w in whole if w[1:] == (0, 0)]]

    def on_device(
        background,
        obs_weight,
        connect,
        live_blocks,
        elem_scale,
        reg_weight,
        iterate,
        residual,
        direction,
        send_nodes,
        send_count,
        ref_stiff,
    ):
        elements = connect.shape[1]
        link = send_nodes.shape[3]
        links = 3 * subs
        nodes = connect.shape[0]
        own_high = background.shape[1] // LANES
        ghost_high = -(-links * link // LANES // 16) * 16
        vmem = pl.BlockSpec(memory_space=pltpu.VMEM)
        smem = pl.BlockSpec(memory_space=pltpu.SMEM)
        hbm = pl.BlockSpec(memory_space=pltpu.HBM)
        partners = sum(len(stage) for stage in stages)
        row = (1, elements)
        operands = (
            background,
            obs_weight.reshape(-1, LANES),
            connect,
            live_blocks,
            elem_scale.reshape(row),
            reg_weight.reshape(row),
            iterate.reshape(row),
            residual.reshape(row),
            direction.reshape(row),
            send_nodes,
            send_count.transpose(0, 2, 1),
            ref_stiff,
        )
        spaces = [pltpu.VMEM] * 9 + [pltpu.SMEM, pltpu.VMEM]
        result = pl.pallas_call(
            functools.partial(kernel, doms, subs, fields, stages),
            out_shape=jax.ShapeDtypeStruct((3,) + row, F32),
            in_specs=[hbm] * 3 + [smem] + [hbm] * 8,
            out_specs=vmem,
            scratch_shapes=[space(x.shape, x.dtype) for space, x in zip(spaces, operands[:3] + operands[4:])]
            + [
                pltpu.VMEM((3, own_high, LANES), F32),
                pltpu.VMEM((3, ghost_high, LANES), F32),
                pltpu.VMEM((6 * own_high, LANES), BF16),
                pltpu.VMEM((6 * ghost_high, LANES), BF16),
                pltpu.VMEM((3 * nodes, elements), F32),
                pltpu.VMEM((3 * nodes, elements), F32),
                pltpu.VMEM((6 * own_high, LANES), F32),
                pltpu.VMEM((6 * ghost_high, LANES), F32),
                pltpu.VMEM((3, own_high, LANES), F32),
                pltpu.VMEM((max(fields - 1, 1), 3, own_high, LANES), F32),
                pltpu.VMEM((links, 3, link), F32),
                pltpu.VMEM((links, 3, link), F32),
                pltpu.VMEM((links, 3, link), F32),
                pltpu.VMEM((links, 3, link), F32),
                pltpu.VMEM((links, 3, link), F32),
                pltpu.VMEM((fields, links, 3, link), F32),
                pltpu.VMEM((len(stages) + 1, 8, LANES), F32),
                pltpu.VMEM((partners, 8, LANES), F32),
                pltpu.SemaphoreType.DMA((11,)),
                pltpu.SemaphoreType.DMA((2, links)),
                pltpu.SemaphoreType.DMA((2, links)),
                pltpu.SemaphoreType.DMA((2, fields, links)),
                pltpu.SemaphoreType.DMA((2, max(fields - 1, 1))),
                pltpu.SemaphoreType.DMA((2, partners)),
            ],
            compiler_params=pltpu.CompilerParams(
                collective_id=0, has_side_effects=True, vmem_limit_bytes=67043328
            ),
        )(*operands)
        outs = pl.pallas_call(
            hand_out,
            out_shape=[jax.ShapeDtypeStruct(row, F32)] * 3,
            in_specs=[vmem],
            out_specs=[hbm] * 3,
            scratch_shapes=[pltpu.SemaphoreType.DMA((3,))],
        )(result)
        return tuple(x.reshape(elements) for x in outs)

    owned = P(("groups", "dom", "sub"))
    element = P(("groups", "dom", "sub", "field"))
    return jax.shard_map(
        on_device,
        mesh=mesh,
        in_specs=(
            P(None, ("groups", "dom", "sub")),
            owned,
            P(None, ("groups", "dom", "sub", "field")),
            element,
            element,
            element,
            element,
            element,
            element,
            P(("groups", "dom", "sub"), None, None, None),
            P(("groups", "dom", "sub"), None, None),
            P(),
        ),
        out_specs=(element, element, element),
        check_vma=False,
    )
```
